32 devices in a mesh: seq: 8 (over z, x), tp: 4 (over y, core).
Axes of the slice: x: 2, y: 2, z: 4, core: 2. Of those that a mesh axis runs over, the one named last changes fastest.
Arguments:
- tree_hidden: bfloat16 [16, 8192], P(None, 'seq'), may hold values from -6 to 6
- query_low: bfloat16 [16, 8192], P('seq', 'tp'), may hold values from -24 to 24
- key_tree_low: bfloat16 [16, 1024], P('seq', 'tp'), may hold values from -20 to 20
- value_tree_low: bfloat16 [16, 1024], P('seq', 'tp'), may hold values from -6 to 6
- cache_keys: bfloat16 [1, 8192, 8, 128], P(None, 'seq', 'tp'), may hold values from -40 to 40
- cache_values: bfloat16 [1, 8192, 8, 128], P(None, 'seq', 'tp'), may hold values from -6 to 6
- cache_lengths: int32 [1], replicated, may hold values from 1024 to 8192
- ancestors: int32 [1, 16, 16], replicated, may hold values from 0 to 1, as said below
- out_weight: bfloat16 [8192, 8192], P('tp', 'seq'), may hold values from -0.0625 to 0.0625
- norm_gain: float32 [8192], P('seq'), may hold values from 0.1 to 1.9
- w_query_up: bfloat16 [8192, 8192], P('seq', 'tp'), may hold values from -0.0625 to 0.0625
- w_key_up: bfloat16 [8192, 1024], P('seq', 'tp'), may hold values from -0.5 to 0.5
- w_value_up: bfloat16 [8192, 1024], P('seq', 'tp'), may hold values from -0.0625 to 0.0625
- retained_keys: bfloat16 [8, 512, 8, 128], P('seq', None, 'tp'), may hold values from -400 to 400
- retained_values: bfloat16 [8, 512, 8, 128], P('seq', None, 'tp'), may hold values from -6 to 6
- retained_index: int32 [8, 512, 8], P('seq', None, 'tp'), may hold values from 0 to 8191
Outputs:
- residual: float32 [16, 8192], P(None, 'seq')
- upper_heads: float32 [16, 8192], P('seq', 'tp')
The draws below stay inside these ranges and needn't reach their ends.
Inputs may be any that keep to these rules, and one draw needn't show every extreme that they name: ancestors[r, i, j] is 1 when node j is node i or an ancestor of node i in request r's tree, else 0; node 0 is the root and every other node's parent has a lower number.
All inputs are finite; a program needn't handle non-finite values.
Results may differ from the reference program's by a relative error of at most 0.04.
Values may be sent and summed in bfloat16 or wider, within the bound.
A program may use at most 64 MiB of HBM per device.

```python
import jax
import jax.numpy as jnp
from jax import lax

D = 8192
HQ = 64
KVH = 8
HD = 128
NODES = 16
GROUP = 8
RET = 4096
R = 1
M = 16
CACHE = 8192
RET_PART = 512


def tree_queries(key):
    drawn = jax.random.normal(jax.random.fold_in(key, 101), (R * NODES, HQ * HD), jnp.float32) * 4.0
    return jnp.clip(drawn, -24.0, 24.0)


def draw_query_low(key, part):
    return tree_queries(key).astype(jnp.bfloat16)


def draw_cache_keys(key, part):
    array_shape = (R, CACHE, KVH, HD)
    key_rows = jnp.clip(jax.random.normal(jax.random.fold_in(key, 103), array_shape, jnp.float32), -5.0, 5.0)
    return key_rows.astype(jnp.bfloat16)


def draw_retained_keys(key, part):
    array_shape = (R * GROUP, RET // GROUP, KVH, HD)
    key_rows = jnp.clip(jax.random.normal(jax.random.fold_in(key, 106), array_shape, jnp.float32) * 4.0, -24.0, 24.0)
    return key_rows.astype(jnp.bfloat16)


def draw_ancestors(key, part):
    random_bits = jax.random.randint(jax.random.fold_in(key, 107), (R, NODES), 0, 1 << 20)
    node_ids = jnp.arange(NODES, dtype=jnp.int32)
    parent_span = jnp.minimum(jnp.maximum(node_ids, 1), 8)
    parents = jnp.maximum(node_ids[None, :] - 1 - random_bits % parent_span[None, :], 0)
    identity = (node_ids[:, None] == node_ids[None, :]).astype(jnp.int32)
    ancestry = jnp.broadcast_to(identity, (R, NODES, NODES))
    request_ids = jnp.arange(R, dtype=jnp.int32)

    def extend(node_index, table):
        parent_row = table[request_ids, parents[:, node_index]]
        new_row = jnp.maximum(parent_row, (node_ids == node_index).astype(jnp.int32)[None, :])
        return table.at[:, node_index].set(new_row)
    return lax.fori_loop(1, NODES, extend, ancestry)


def set_ends(result, rng, least, largest):
    place = [jax.random.randint(jax.random.fold_in(rng, axis), (), 0, length) for axis, length in enumerate(result.shape)]
    widest = result.shape.index(max(result.shape))
    neighbour = place[:widest] + [(place[widest] + 1) % result.shape[widest]] + place[widest + 1:]
    return result.at[tuple(place)].set(least).at[tuple(neighbour)].set(largest)


def levels(rng, extent, pieces, low, top_value):
    gain = 1.0
    for dim, blocks in pieces:
        heights = jax.random.uniform(jax.random.fold_in(jax.random.fold_in(rng, 6), dim), (blocks,), jnp.float32, low / len(pieces), top_value / len(pieces))
        gain = gain * jnp.repeat(jnp.exp(heights), extent[dim] // blocks).reshape((-1,) + (1,) * (len(extent) - 1 - dim))
    return gain


def normal_values(rng, shape, width, reach, split=(), kind=jnp.bfloat16):
    loudness = levels(rng, shape, split, -0.22, 0.18) if split else 1.0
    values = jax.random.normal(rng, shape, jnp.float32) * width * loudness
    return jnp.minimum(jnp.maximum(values, -reach), reach).astype(kind)


def setup_inputs(seed: int = 0) -> dict:
    key_list = jax.random.split(jax.random.key(seed), 17)
    return {
        "tree_hidden": normal_values(key_list[0], (M, D), 1.0, 6.0, ((1, 8),)),
        "query_low": draw_query_low(jax.random.fold_in(key_list[16], 71), 0),
        "key_tree_low": normal_values(key_list[2], (M, KVH * HD), 3.5, 20.0, ((0, 8), (1, 4))),
        "value_tree_low": normal_values(key_list[3], (M, KVH * HD), 1.0, 6.0, ((0, 8), (1, 4))),
        "cache_keys": draw_cache_keys(jax.random.fold_in(key_list[16], 71), 0),
        "cache_values": normal_values(key_list[5], (R, CACHE, KVH, HD), 1.0, 6.0, ((1, 8), (2, 4))),
        "cache_lengths": jax.random.randint(key_list[6], (R,), CACHE // 8, CACHE + 1).astype(jnp.int32),
        "ancestors": draw_ancestors(jax.random.fold_in(key_list[16], 71), 0),
        "out_weight": normal_values(key_list[8], (HQ * HD, D), (HQ * HD) ** -0.5, 0.0625, ((0, 4), (1, 8))),
        "norm_gain": jnp.clip(1.0 + 0.18 * jax.random.normal(key_list[9], (D,), jnp.float32), 0.1, 1.9),
        "w_query_up": normal_values(key_list[10], (D, HQ * HD), D ** -0.5, 0.0625, ((0, 8), (1, 4))),
        "w_key_up": normal_values(key_list[11], (D, KVH * HD), (D // 64) ** -0.5, 0.5, ((0, 8), (1, 4))),
        "w_value_up": normal_values(key_list[12], (D, KVH * HD), D ** -0.5, 0.0625, ((0, 8), (1, 4))),
        "retained_keys": draw_retained_keys(jax.random.fold_in(key_list[16], 71), 0),
        "retained_values": normal_values(key_list[14], (R * GROUP, RET_PART, KVH, HD), 1.0, 6.0, ((0, 8), (2, 4))),
        "retained_index": set_ends(jax.random.randint(key_list[15], (R * GROUP, RET_PART, KVH), 0, CACHE), jax.random.fold_in(key_list[15], 1), 0, CACHE - 1).astype(jnp.int32),
    }


masked_score = -1e+30
norm_epsilon = 1e-05

def joint_attend(query_rows, far_keys, far_values, far_allowed, near_keys, near_values, near_mask):
    row_count = query_rows.shape[0]
    group_size = HQ // KVH
    queries = query_rows.astype(jnp.float32).reshape(row_count, KVH, group_size, HD).transpose(1, 0, 2, 3)
    near_key_rows = near_keys.astype(jnp.float32).reshape(-1, KVH, HD).transpose(1, 0, 2)
    near_value_rows = near_values.astype(jnp.float32).reshape(-1, KVH, HD).transpose(1, 0, 2)
    near_usable = near_mask > 0

    def one_head(operands):
        head_query, key_rows, value_rows, usable, tree_keys, tree_values = operands
        far_scores = jnp.einsum('ngd,cd->ngc', head_query, key_rows.astype(jnp.float32)) * HD ** (-0.5)
        near_scores = jnp.einsum('ngd,md->ngm', head_query, tree_keys) * HD ** (-0.5)
        scores = jnp.concatenate([far_scores, near_scores], axis=-1)
        allowed = jnp.concatenate([jnp.broadcast_to(usable[None, None, :], far_scores.shape), jnp.broadcast_to(near_usable[:, None, :], near_scores.shape)], axis=-1)
        masked = jnp.where(allowed, scores, masked_score)
        highest = lax.optimization_barrier(jnp.max(masked, axis=-1, keepdims=True))
        weights = jnp.where(allowed, jnp.exp(masked - highest), 0.0)
        weight_sum = lax.optimization_barrier(jnp.sum(weights, axis=-1, keepdims=True))
        rounded = lax.optimization_barrier(weights.astype(jnp.bfloat16)).astype(jnp.float32)
        both_values = jnp.concatenate([value_rows.astype(jnp.float32), tree_values], axis=0)
        return jnp.einsum('ngc,cd->ngd', rounded, both_values) / weight_sum
    blended = lax.map(one_head, (queries, far_keys.transpose(1, 0, 2), far_values.transpose(1, 0, 2), far_allowed.T, near_key_rows, near_value_rows))
    return blended.transpose(1, 0, 2, 3).reshape(row_count, HQ * HD).astype(jnp.float32)

def reference(tree_hidden, query_low, key_tree_low, value_tree_low, cache_keys, cache_values, cache_lengths, ancestors, out_weight, norm_gain, w_query_up, w_key_up, w_value_up, retained_keys, retained_values, retained_index):
    positions = jnp.arange(CACHE, dtype=jnp.int32)

    def lower_request(operands):
        query_rows, key_rows, value_rows, seq_length, tree_keys, tree_values, tree_mask = operands
        usable = jnp.broadcast_to((positions < seq_length)[:, None], (CACHE, KVH))
        return joint_attend(query_rows, key_rows, value_rows, usable, tree_keys, tree_values, tree_mask).astype(jnp.bfloat16)
    lower = lax.map(lower_request, (query_low.reshape(R, NODES, HQ * HD), cache_keys, cache_values, cache_lengths, key_tree_low.reshape(R, NODES, KVH * HD), value_tree_low.reshape(R, NODES, KVH * HD), ancestors)).reshape(R * NODES, HQ * HD)
    summed = jnp.dot(lower, out_weight, preferred_element_type=jnp.float32)
    residual = tree_hidden.astype(jnp.float32) + summed
    inverse = lax.rsqrt(lax.optimization_barrier(jnp.mean(residual * residual, axis=1, keepdims=True)) + norm_epsilon)
    normed = (residual * inverse * norm_gain[None, :]).astype(jnp.bfloat16)
    query_up = jnp.dot(normed, w_query_up, preferred_element_type=jnp.float32).astype(jnp.bfloat16)
    key_up = jnp.dot(normed, w_key_up, preferred_element_type=jnp.float32).astype(jnp.bfloat16)
    value_up = jnp.dot(normed, w_value_up, preferred_element_type=jnp.float32).astype(jnp.bfloat16)

    def upper_request(operands):
        query_rows, key_rows, value_rows, positions_kept, seq_length, tree_keys, tree_values, tree_mask = operands
        return joint_attend(query_rows, key_rows, value_rows, positions_kept < seq_length, tree_keys, tree_values, tree_mask)
    upper = lax.map(upper_request, (query_up.reshape(R, NODES, HQ * HD), retained_keys.reshape(R, RET, KVH, HD), retained_values.reshape(R, RET, KVH, HD), retained_index.reshape(R, RET, KVH), cache_lengths, key_up.reshape(R, NODES, KVH * HD), value_up.reshape(R, NODES, KVH * HD), ancestors)).reshape(R * NODES, HQ * HD)
    return (residual, upper)
```

```python
import functools
import math

import jax
import jax.numpy as jnp
from jax import lax
from jax.experimental import pallas as pl
from jax.experimental.pallas import tpu as pltpu
from jax.sharding import PartitionSpec as P

MESH = pl.DeviceIdType.MESH
F32 = jnp.float32
BF16 = jnp.bfloat16
masked_score = -1e30
lowest_high = -1e29
norm_epsilon = 1e-05
last_last = (((1,), (1,)), ((), ()))


def contract_last(a, b):
    return lax.dot_general(a, b, last_last, preferred_element_type=F32)


def flip(index, bits):
    result = index
    bit = 1
    while bit <= bits:
        if bits & bit:
            result = result + (1 - 2 * lax.rem(lax.div(index, bit), 2)) * bit
        bit *= 2
    return result


def kernel(
    sizes,
    lens_hbm,
    q_hbm,
    k_hbm,
    v_hbm,
    ck_hbm,
    cv_hbm,
    anc_hbm,
    ow_hbm,
    hid_hbm,
    gain_hbm,
    ridx_hbm,
    rk_hbm,
    rv_hbm,
    wk_hbm,
    wv_hbm,
    wq_hbm,
    res_ref,
    up_ref,
    lens_ref,
    q_ref,
    k_ref,
    v_ref,
    ck,
    cv,
    anc_ref,
    ow,
    hid_ref,
    gain_ref,
    ridx_ref,
    rk,
    rv,
    weight,
    form,
    wide,
    ckeys,
    cvals,
    rkeys,
    rvals,
    bias_ref,
    low,
    part,
    gpart,
    tops,
    heads,
    terms,
    proj,
    gproj,
    square,
    gsquare,
    upper,
    upart,
    ugpart,
    load_sem,
    weight_sem,
    send_sem,
    recv_sem,
):
    S, T, R, own, kv, g, hd = sizes
    G = S // R
    H = G // 2
    M = S * own
    rows = own * g
    nodes = G * own
    lanes = nodes * g
    per_k = H // kv
    slab = hd // per_k
    qcols = kv * g * hd // H
    kcols = 2 * kv * hd // H
    hub_heads = qcols // hd
    scale = hd ** (-0.5)
    sharp = scale * math.log2(math.e)
    width = S * hid_ref.shape[1]
    half = hid_ref.shape[1] // 2
    me = lax.axis_index("seq")
    tp = lax.axis_index("tp")
    request = lax.div(me, G)
    base = request * G
    place = me - base
    first_hub = G // 4
    slot = place - first_hub
    is_hub = jnp.logical_and(place >= first_hub, place < first_hub + H)
    side = lax.div(place, G // 2)
    lane_of = lax.rem(place, per_k)

    def hub(r, c):
        return r * G + first_hub + c

    barrier = pltpu.get_barrier_semaphore()
    for d in range(1, S):
        pl.semaphore_signal(
            barrier, inc=1, device_id={"seq": flip(me, d)}, device_id_type=MESH
        )
    for d in range(1, T):
        pl.semaphore_signal(
            barrier, inc=1, device_id={"tp": flip(tp, d)}, device_id_type=MESH
        )

    loads = []
    for i, (src, dst) in enumerate(
        (
            (q_hbm, q_ref),
            (k_hbm, k_ref),
            (v_hbm, v_ref),
            (lens_hbm, lens_ref),
            (ck_hbm, ck),
            (cv_hbm, cv),
            (anc_hbm, anc_ref),
            (ow_hbm, ow),
            (rk_hbm, rk),
            (rv_hbm, rv),
            (ridx_hbm, ridx_ref),
            (hid_hbm, hid_ref),
            (gain_hbm, gain_ref),
        )
    ):
        copy = pltpu.make_async_copy(src, dst, load_sem.at[i])
        copy.start()
        loads.append(copy)
    weights = []
    for c in range(H):
        source, at = (wk_hbm, c) if c < H // 2 else (wv_hbm, c - H // 2)
        for i, (src, dst) in enumerate(
            (
                (wq_hbm.at[:, pl.ds(c * qcols, qcols)], weight.at[c, :, pl.ds(0, qcols)]),
                (source.at[:, pl.ds(at * kcols, kcols)], weight.at[c, :, pl.ds(qcols, kcols)]),
            )
        ):
            copy = pltpu.make_async_copy(src, dst, weight_sem.at[c, i])
            copy.start()
            weights.append(copy)

    sent = []

    def send(phase, at, src, dst, to, target, when=None):
        copy = pltpu.make_async_remote_copy(
            src_ref=src,
            dst_ref=dst,
            send_sem=send_sem.at[phase, at],
            recv_sem=recv_sem.at[phase, to],
            device_id=target,
            device_id_type=MESH,
        )
        if when is None:
            copy.start()
        else:
            pl.when(when)(copy.start)
        sent.append((when, copy))

    def arrive(phase, source, there, target, when=None):
        copy = pltpu.make_async_remote_copy(
            src_ref=there,
            dst_ref=there,
            send_sem=send_sem.at[phase, 0],
            recv_sem=recv_sem.at[phase, source],
            device_id=target,
            device_id_type=MESH,
        )
        if when is None:
            copy.wait_recv()
        else:
            pl.when(when)(copy.wait_recv)

    row_a = lax.broadcasted_iota(jnp.int32, (lanes, lanes), 0)
    col_a = lax.broadcasted_iota(jnp.int32, (lanes, lanes), 1)

    def one_hot(where):
        return jnp.where(where, 1.0, 0.0).astype(BF16)

    form[kv] = jnp.zeros(form.shape[1:], F32)
    for i in range(3):
        loads[i].wait()
    q_rows = q_ref[...].astype(F32)
    k_rows = k_ref[...].astype(F32)
    v_rows = v_ref[...].astype(F32)
    for k in range(kv):
        for j in range(g):
            h = k * g + j
            form[k, pl.ds(j, own, stride=g), :] = q_rows[:, h * hd : (h + 1) * hd]
        form[kv, pl.ds(k, own, stride=g), :] = k_rows[:, k * hd : (k + 1) * hd]
        form[kv, pl.ds(kv + k, own, stride=g), :] = v_rows[:, k * hd : (k + 1) * hd]
    for k in range(kv + 1):
        low[me, k] = form[k, :rows, :].astype(BF16)

    pl.semaphore_wait(barrier, S - 1 + T - 1)

    for d in reversed(range(1, S)):
        own_q = low.at[me, pl.ds(0, kv)]
        send(0, d, own_q, own_q, me, {"seq": flip(me, d)})
    for c in range(H):
        own_kv = low.at[me, pl.ds(kv, 1)]
        target = hub(request, c)
        send(2, c, own_kv, own_kv, me, {"seq": target}, target != me)

    for i in range(3, 7):
        loads[i].wait()
    columns = ckeys.shape[2]
    first = me * columns
    position = lax.broadcasted_iota(jnp.int32, (columns, hd), 0) + first
    for r in range(R):
        wide[: columns * kv] = ck[r].astype(F32)
        allowed = jnp.where(position < lens_ref[r], 0.0, masked_score).astype(BF16)
        for k in range(kv):
            ckeys[r, k, :, :hd] = wide[pl.ds(k, columns, stride=kv), :].astype(BF16)
            ckeys[r, k, :, hd:] = allowed
        wide[: columns * kv] = cv[r].astype(F32)
        for k in range(kv):
            cvals[r, k, :hd, :] = wide[pl.ds(k, columns, stride=kv), :].T.astype(BF16)
            cvals[r, k, hd:, :] = jnp.ones((cvals.shape[2] - hd, columns), BF16)

    lead = one_hot(lax.broadcasted_iota(jnp.int32, (lanes, hd), 1) == 0)
    row_s = lax.broadcasted_iota(jnp.int32, (16, lanes), 0)
    for d in range(1, S):
        source = flip(me, d)
        arrive(0, source, low.at[source, pl.ds(0, kv)], {"seq": source})

    for r in range(R):
        for step in range(kv):
            k = lax.rem(side + kv - 1 - step, kv)
            queries = low[pl.ds(r * G, G), k].reshape(lanes, hd)
            queries = jnp.concatenate([queries, lead], axis=1)
            scores = contract_last(ckeys[r, k], queries)
            high = jnp.maximum(jnp.max(scores, axis=0, keepdims=True), lowest_high)
            high = high.astype(BF16).astype(F32)
            mass = jnp.exp2((scores - high) * sharp).astype(BF16)
            blend = jnp.dot(cvals[r, k], mass, preferred_element_type=F32)
            total = blend[hd : hd + 1]
            coarse = total.astype(BF16).astype(F32)
            stats = jnp.where(row_s == 1, coarse, jnp.where(row_s == 2, total - coarse, 0.0))
            stats = jnp.where(row_s == 0, high, stats).astype(BF16)
            for h in range(per_k):
                part[r, k * per_k + h, :slab, :] = blend[h * slab : (h + 1) * slab].astype(BF16)
                part[r, k * per_k + h, slab:, :] = stats
            for d in reversed(range(per_k)):
                c = k * per_k + lax.rem(lane_of + d, per_k)
                target = hub(r, c)
                send(
                    1,
                    (r * kv + step) * per_k + d,
                    part.at[r, c],
                    gpart.at[me],
                    me,
                    {"seq": target},
                    target != me,
                )

    @pl.when(is_hub)
    def _():
        k = lax.div(slot, per_k)
        part_of = lax.rem(slot, per_k)
        ancestry = anc_ref[request].astype(F32).astype(BF16)
        spread = one_hot(
            lax.div(lax.broadcasted_iota(jnp.int32, (lanes, nodes), 0), g)
            == lax.broadcasted_iota(jnp.int32, (lanes, nodes), 1)
        )
        mask = jnp.dot(spread, ancestry, preferred_element_type=F32).astype(BF16)
        small = one_hot(
            lax.broadcasted_iota(jnp.int32, (nodes, nodes), 0)
            == lax.broadcasted_iota(jnp.int32, (nodes, nodes), 1)
        )
        mask = contract_last(small, mask)
        for d in range(1, G):
            source = base + flip(place, d)
            arrive(2, source, low.at[source, pl.ds(kv, 1)], {"seq": source})
        form[kv, :lanes, :] = low[pl.ds(base, G), kv].reshape(lanes, hd).astype(F32)
        keys = form[kv, pl.ds(k, nodes, stride=g), :].astype(BF16)
        values = form[kv, pl.ds(kv + k, nodes, stride=g), :].astype(BF16)
        scores = contract_last(keys, low[pl.ds(base, G), k].reshape(lanes, hd))
        scores = jnp.where(mask > 0.5, scores, masked_score)
        near_high = jnp.max(scores, axis=0, keepdims=True)
        mass = jnp.exp2((scores - near_high) * sharp)
        near_total = jnp.sum(mass, axis=0, keepdims=True)
        turned = contract_last(one_hot(row_a == col_a)[:hd, :hd], values).astype(BF16)
        wide[:hd] = jnp.dot(turned, mass.astype(BF16), preferred_element_type=F32)
        near = wide[pl.ds(pl.multiple_of(part_of * slab, slab), slab), :]
        gpart[me] = part[request, slot]
        for d in range(1, S):
            source = flip(me, d)
            arrive(1, source, gpart.at[source], {"seq": source})
        for s in range(S):
            tops[s * 16 : (s + 1) * 16] = gpart[s, slab:].astype(F32)
        highs = tops[pl.ds(0, S, stride=16), :]
        totals = tops[pl.ds(1, S, stride=16), :] + tops[pl.ds(2, S, stride=16), :]
        top = jnp.maximum(jnp.max(highs, axis=0, keepdims=True), near_high)
        factors = jnp.exp2((highs - top) * sharp)
        late = jnp.exp2((near_high - top) * sharp)
        total = jnp.sum(factors * totals, axis=0, keepdims=True) + near_total * late
        acc = near * late
        for s in range(S):
            acc = acc + gpart[s, :slab].astype(F32) * factors[s : s + 1]
        heads[request, slot] = (acc * (1.0 / total)).astype(BF16)

    for d in reversed(range(1, S)):
        done = heads.at[request, slot]
        send(3, d, done, done, me, {"seq": flip(me, d)}, is_hub)

    entries = rkeys.shape[1]
    for i in range(7, 11):
        loads[i].wait()
    wide[: entries * kv] = rk[...].astype(F32)
    for k in range(kv):
        rkeys[k] = wide[pl.ds(k, entries, stride=kv), :].astype(BF16)
    wide[: entries * kv] = rv[...].astype(F32)
    for k in range(kv):
        rvals[k, :, :hd] = wide[pl.ds(k, entries, stride=kv), :].astype(BF16)
        rvals[k, :, hd:] = jnp.ones((entries, hd), BF16)
        kept = jnp.where(ridx_ref[k : k + 1, :] < lens_ref[request], 0.0, masked_score)
        bias_ref[k] = jnp.broadcast_to(kept, bias_ref.shape[1:])
    mask_rows = []
    for r in range(own):
        row = anc_ref[request, pl.ds(place * own + r, 1), :]
        mask_rows.append(jnp.broadcast_to(row, (g, nodes)))
    tree_mask = jnp.concatenate(mask_rows, axis=0) > 0
    order = one_hot(
        jnp.logical_and(
            lax.rem(row_a, nodes) == lax.div(col_a, g),
            lax.div(row_a, nodes) == lax.rem(col_a, g),
        )
    )

    summed = None
    for step in range(kv):
        k = lax.rem(side + step, kv)
        lower = []
        for r in range(R):
            for d in range(per_k):
                c = k * per_k + lax.rem(lane_of + d, per_k)
                source = hub(r, c)
                arrive(3, source, heads.at[r, c], {"seq": source}, source != me)
            turned = heads[r, pl.ds(k * per_k, per_k)].reshape(hd, lanes)
            turned = contract_last(order, turned).astype(BF16)
            lower.append(
                jnp.concatenate(
                    [turned[j * nodes : (j + 1) * nodes] for j in range(g)], axis=1
                )
            )
        lower = lower[0] if R == 1 else jnp.concatenate(lower, axis=0)
        depth = g * hd
        start = pl.multiple_of(k * depth, depth)
        if step < kv - 1:
            more = jnp.dot(lower, ow[pl.ds(start, depth), :], preferred_element_type=F32)
            summed = more if summed is None else summed + more
        else:
            for p in range(2):
                more = jnp.dot(
                    lower,
                    ow[pl.ds(start, depth), p * half : (p + 1) * half],
                    preferred_element_type=F32,
                )
                if summed is not None:
                    more = more + summed[:, p * half : (p + 1) * half]
                terms[tp, p] = more.astype(BF16)
                for d in reversed(range(1, T)):
                    mine = terms.at[tp, p]
                    send(4, p * T + d, mine, mine, p * T + tp, {"tp": flip(tp, d)})
    loads[11].wait()
    loads[12].wait()
    residual = []
    for p in range(2):
        for d in range(1, T):
            source = flip(tp, d)
            arrive(4, p * T + source, terms.at[source, p], {"tp": source})
        summed = terms[0, p].astype(F32)
        for t in range(1, T):
            summed = summed + terms[t, p].astype(F32)
        residual.append(hid_ref[:, p * half : (p + 1) * half].astype(F32) + summed)
    residual = jnp.concatenate(residual, axis=1)

    squares = jnp.broadcast_to(jnp.sum(residual * residual, axis=1, keepdims=True), (M, hd))
    coarse = squares.astype(BF16).astype(F32)
    lane = lax.broadcasted_iota(jnp.int32, (M, hd), 1)
    squares = jnp.where(lane < hd // 2, coarse, squares - coarse).astype(BF16)
    for r in range(R):
        square[r] = squares[r * nodes : (r + 1) * nodes]
        for c in range(H):
            target = hub(r, c)
            send(
                9, r * H + c, square.at[r], gsquare.at[me], me, {"seq": target}, target != me
            )
    for copy in weights:
        copy.wait()
    scaled = (residual * gain_ref[...]).astype(BF16)
    for step in range(kv):
        for d in reversed(range(per_k)):
            c = lax.rem(side + kv - 1 - step, kv) * per_k + lax.rem(lane_of + d, per_k)
            out = jnp.dot(scaled, weight[c], preferred_element_type=F32).astype(BF16)
            for r in range(R):
                proj[r, c] = out[r * nodes : (r + 1) * nodes]
                target = hub(r, c)
                send(
                    5,
                    (r * kv + step) * per_k + d,
                    proj.at[r, c],
                    gproj.at[me],
                    me,
                    {"seq": target},
                    target != me,
                )
    res_ref[...] = residual

    @pl.when(is_hub)
    def _():
        gsquare[me] = square[request]
        gproj[me] = proj[request, slot]
        for d in range(1, S):
            source = flip(me, d)
            arrive(9, source, gsquare.at[source], {"seq": source})
        total = gsquare[0].astype(F32)
        for s in range(1, S):
            total = total + gsquare[s].astype(F32)
        total = total + pltpu.roll(total, hd // 2, 1)
        inverse = lax.rsqrt(total / width + norm_epsilon)
        for d in range(1, S):
            source = flip(me, d)
            arrive(5, source, gproj.at[source], {"seq": source})
        for t in range((qcols + kcols) // hd):
            at = slice(t * hd, (t + 1) * hd)
            total = gproj[0, :, at].astype(F32)
            for s in range(1, S):
                total = total + gproj[s, :, at].astype(F32)
            upper[slot, :, at] = (total * inverse).astype(BF16)

    for d in reversed(range(1, G)):
        mine = upper.at[slot]
        send(6, d, mine, mine, me, {"seq": base + flip(place, d)}, is_hub)

    spot = lax.broadcasted_iota(jnp.int32, (lanes, hd), 1)
    third = hd // 4

    def pack_stats(high, total):
        packed = jnp.where(jnp.bitwise_and(spot, 1) == 0, high, total)
        coarse = packed.astype(BF16).astype(F32)
        rest = packed - coarse
        middle = rest.astype(BF16).astype(F32)
        fine = rest - middle
        packed = jnp.where(spot < third, coarse, jnp.where(spot < 2 * third, middle, fine))
        return jnp.where(spot < 3 * third, packed, 0.0)

    def unpack_stats(block):
        packed = block.astype(F32)
        return (packed + pltpu.roll(packed, hd - third, 1)) + pltpu.roll(
            packed, hd - 2 * third, 1
        )

    pick = one_hot(
        jnp.logical_and(
            lax.div(lax.broadcasted_iota(jnp.int32, (rows, lanes), 0), g) + place * own
            == lax.rem(lax.broadcasted_iota(jnp.int32, (rows, lanes), 1), nodes),
            lax.rem(lax.broadcasted_iota(jnp.int32, (rows, lanes), 0), g)
            == lax.div(lax.broadcasted_iota(jnp.int32, (rows, lanes), 1), nodes),
        )
    )

    def upper_queries(k):
        tiles = []
        for j in range(g):
            tile = upper[k * per_k + j // hub_heads]
            tiles.append(tile[:, (j % hub_heads) * hd : (j % hub_heads + 1) * hd])
        return jnp.concatenate(tiles, axis=0)

    for step in range(kv):
        k = lax.rem(side + step, kv)
        for d in range(per_k):
            c = k * per_k + lax.rem(lane_of + d, per_k)
            source = hub(request, c)
            arrive(6, source, upper.at[c], {"seq": source}, source != me)
        scores = contract_last(upper_queries(k), rkeys[k]) + bias_ref[k, 0:1, :]
        high = jnp.maximum(jnp.max(scores, axis=1, keepdims=True), lowest_high)
        mass = jnp.exp2((scores - high) * sharp).astype(BF16)
        blend = jnp.dot(mass, rvals[k], preferred_element_type=F32)
        form[0, :lanes, :] = blend[:, :hd]
        form[1, :lanes, :] = pack_stats(high, blend[:, hd:])
        for a in range(G):
            for i in range(2):
                tile = [form[i, pl.ds(a * own + b, g, stride=nodes), :] for b in range(own)]
                upart[a, k, i * rows : (i + 1) * rows, :] = jnp.concatenate(tile, axis=0).astype(
                    BF16
                )
        for d in reversed(range(1, G)):
            target = flip(place, d)
            send(
                7,
                step * S + d,
                upart.at[target, k],
                ugpart.at[place, k],
                step * S + place,
                {"seq": base + target},
            )
    ugpart[place] = upart[place]

    trees = []
    for k in range(kv):
        queries = jnp.dot(pick, upper_queries(k), preferred_element_type=F32).astype(BF16)
        keys = upper[(k * hd) // kcols][:, qcols:]
        values = upper[H // 2 + (k * hd) // kcols][:, qcols:]
        scores = jnp.where(tree_mask, contract_last(queries, keys), masked_score)
        high = jnp.max(scores, axis=1, keepdims=True)
        mass = jnp.exp2((scores - high) * sharp)
        total = jnp.sum(mass, axis=1, keepdims=True)
        trees.append((jnp.dot(mass.astype(BF16), values, preferred_element_type=F32), high, total))
    for step in range(kv):
        for d in range(1, G):
            source = flip(place, d)
            k = lax.rem(lax.div(source, G // 2) + step, kv)
            arrive(7, step * S + source, ugpart.at[source, k], {"seq": base + source})
    for k in range(kv):
        blend, high, total = trees[k]
        stats = [unpack_stats(ugpart[s, k, rows:]) for s in range(G)]
        top = jnp.maximum(functools.reduce(jnp.maximum, stats)[:, 0:1], high)
        late = jnp.exp2((high - top) * sharp)
        acc = blend * late
        whole = total * late
        mass = jnp.zeros((rows, hd), F32)
        for s in range(G):
            factor = jnp.exp2((stats[s] - top) * sharp)
            acc = acc + ugpart[s, k, :rows].astype(F32) * factor[:, 0:1]
            mass = mass + pltpu.roll(stats[s], hd - 1, 1) * factor
        form[k, :rows, :] = acc / (whole + mass[:, 0:1])
        for j in range(g):
            h = k * g + j
            up_ref[:, h * hd : (h + 1) * hd] = form[k, pl.ds(j, own, stride=g), :]
    for when, copy in sent:
        if when is None:
            copy.wait_send()
        else:
            pl.when(when)(copy.wait_send)


def shards(
    tree_hidden,
    query_low,
    key_tree_low,
    value_tree_low,
    cache_keys,
    cache_values,
    cache_lengths,
    ancestors,
    out_weight,
    norm_gain,
    w_query_up,
    w_key_up,
    w_value_up,
    retained_keys,
    retained_values,
    retained_index,
):
    S = lax.axis_size("seq")
    T = lax.axis_size("tp")
    R, part, kv, hd = cache_keys.shape
    own, row_width = query_low.shape
    g = row_width // (kv * hd)
    G = S // R
    M = S * own
    rows = own * g
    features = tree_hidden.shape[1]
    entries = retained_keys.shape[1] * kv
    ck = cache_keys.reshape(R, part * kv, hd)
    cv = cache_values.reshape(R, part * kv, hd)
    rk = retained_keys.reshape(entries, hd)
    rv = retained_values.reshape(entries, hd)
    ridx = retained_index[0].T
    gain = norm_gain.reshape(1, features)
    vmem = pl.BlockSpec(memory_space=pltpu.VMEM)
    hbm = pl.BlockSpec(memory_space=pl.ANY)
    H = G // 2
    columns = part
    big = (
        query_low,
        key_tree_low,
        value_tree_low,
        ck,
        cv,
        ancestors,
        out_weight,
        tree_hidden,
        gain,
        ridx,
        rk,
        rv,
    )
    cols = (kv * g * hd + 2 * kv * hd) // H
    nodes = G * own
    lanes = nodes * g
    slab = hd * kv // H
    outs = pl.pallas_call(
        functools.partial(kernel, (S, T, R, own, kv, g, hd)),
        out_shape=(
            pltpu.VMEM((M, features), F32),
            pltpu.VMEM((own, row_width), F32),
        ),
        in_specs=[hbm] * (4 + len(big)),
        out_specs=(vmem, vmem),
        scratch_shapes=[pltpu.SMEM((R,), jnp.int32)]
        + [pltpu.VMEM(x.shape, x.dtype) for x in big]
        + [
            pltpu.VMEM((H, features, cols), BF16),
            pltpu.VMEM((kv + 1, lanes, hd), F32),
            pltpu.VMEM((max(columns * kv, entries), hd), F32),
            pltpu.VMEM((R, kv, columns, 2 * hd), BF16),
            pltpu.VMEM((R, kv, hd + 16, columns), BF16),
            pltpu.VMEM((kv, entries // kv, hd), BF16),
            pltpu.VMEM((kv, entries // kv, 2 * hd), BF16),
            pltpu.VMEM((kv, 8, entries // kv), F32),
            pltpu.VMEM((S, kv + 1, rows, hd), BF16),
            pltpu.VMEM((R, H, slab + 16, lanes), BF16),
            pltpu.VMEM((S, slab + 16, lanes), BF16),
            pltpu.VMEM((S * 16, lanes), F32),
            pltpu.VMEM((R, H, slab, lanes), BF16),
            pltpu.VMEM((T, 2, M, features // 2), BF16),
            pltpu.VMEM((R, H, nodes, cols), BF16),
            pltpu.VMEM((S, nodes, cols), BF16),
            pltpu.VMEM((R, nodes, hd), BF16),
            pltpu.VMEM((S, nodes, hd), BF16),
            pltpu.VMEM((H, nodes, cols), BF16),
            pltpu.VMEM((G, kv, 2 * rows, hd), BF16),
            pltpu.VMEM((G, kv, 2 * rows, hd), BF16),
            pltpu.SemaphoreType.DMA((1 + len(big),)),
            pltpu.SemaphoreType.DMA((H, 2)),
            pltpu.SemaphoreType.DMA((10, 2 * max(S, T))),
            pltpu.SemaphoreType.DMA((10, 2 * max(S, T))),
        ],
        compiler_params=pltpu.CompilerParams(
            collective_id=0, has_side_effects=True, vmem_limit_bytes=56 * 1024 * 1024
        ),
        name="two_layers",
    )(
        cache_lengths,
        *big,
        w_key_up,
        w_value_up,
        w_query_up,
    )

    def settle(a_ref, b_ref, c_ref, d_ref):
        c_ref[...] = a_ref[...]
        d_ref[...] = b_ref[...]

    return pl.pallas_call(
        settle,
        out_shape=tuple(jax.ShapeDtypeStruct(x.shape, x.dtype) for x in outs),
        in_specs=[vmem] * 2,
        out_specs=(vmem, vmem),
        name="settle",
    )(*[pltpu.with_memory_space_constraint(x, pltpu.VMEM) for x in outs])


def solution(mesh):
    return jax.shard_map(
        shards,
        mesh=mesh,
        in_specs=(
            P(None, "seq"),
            P("seq", "tp"),
            P("seq", "tp"),
            P("seq", "tp"),
            P(None, "seq", "tp", None),
            P(None, "seq", "tp", None),
            P(),
            P(),
            P("tp", "seq"),
            P("seq"),
            P("seq", "tp"),
            P("seq", "tp"),
            P("seq", "tp"),
            P("seq", None, "tp", None),
            P("seq", None, "tp", None),
            P("seq", None, "tp"),
        ),
        out_specs=(P(None, "seq"), P("seq", "tp")),
        check_vma=False,
    )
```

```python
import functools
import math

import jax
import jax.numpy as jnp
from jax import lax
from jax.experimental import pallas as pl
from jax.experimental.pallas import tpu as pltpu
from jax.sharding import PartitionSpec as P

MESH = pl.DeviceIdType.MESH
F32 = jnp.float32
BF16 = jnp.bfloat16
masked_score = -1e30
lowest_high = -1e29
norm_epsilon = 1e-05
last_last = (((1,), (1,)), ((), ()))


def contract_last(a, b):
    return lax.dot_general(a, b, last_last, preferred_element_type=F32)


def bits_of(index, count):
    found = []
    bit = 1
    while 2 * bit < count:
        bit *= 2
    while bit and count > 1:
        there = jnp.where(index >= bit, 1, 0)
        index = index - there * bit
        found.append((bit, there))
        bit //= 2
    return found


def flips(index, count):
    steps = [(bit, (1 - 2 * there) * bit) for bit, there in bits_of(index, count)]
    result = []
    for d in range(count):
        other = index
        for bit, step in steps:
            if d & bit:
                other = other + step
        result.append(other)
    return result


def turn(index, step, count):
    if step % count == 0:
        return index
    if count == 2:
        return 1 - index
    return lax.rem(index + step, count)


def kernel(
    sizes,
    lens_hbm,
    q_hbm,
    k_hbm,
    v_hbm,
    ck_hbm,
    cv_hbm,
    anc_hbm,
    ow_hbm,
    hid_hbm,
    gain_hbm,
    ridx_hbm,
    rk_hbm,
    rv_hbm,
    wk_hbm,
    wv_hbm,
    wq_hbm,
    res_ref,
    up_ref,
    lens_ref,
    q_ref,
    k_ref,
    v_ref,
    ck,
    cv,
    anc_ref,
    ow,
    hid_ref,
    gain_ref,
    ridx_ref,
    rk,
    rv,
    weight,
    form,
    wide,
    ckeys,
    cvals,
    rkeys,
    rvals,
    bias_ref,
    low,
    part,
    gpart,
    tops,
    heads,
    terms,
    proj,
    gproj,
    square,
    gsquare,
    upper,
    upart,
    ugpart,
    load_sem,
    weight_sem,
    send_sem,
    recv_sem,
):
    S, T, R, own, kv, g, hd = sizes
    G = S // R
    H = G // 2
    M = S * own
    rows = own * g
    nodes = G * own
    lanes = nodes * g
    per_k = H // kv
    slab = hd // per_k
    qcols = kv * g * hd // H
    kcols = 2 * kv * hd // H
    hub_heads = qcols // hd
    scale = hd ** (-0.5)
    sharp = scale * math.log2(math.e)
    width = S * hid_ref.shape[1]
    half = hid_ref.shape[1] // 2
    me = lax.axis_index("seq")
    tp = lax.axis_index("tp")
    request = 0 if R == 1 else lax.div(me, G)
    base = request * G
    place = me - base
    peers = flips(me, S)
    mates = flips(place, G)
    twins = flips(tp, T)
    first_hub = G // 4
    slot = place - first_hub
    is_hub = jnp.logical_and(place >= first_hub, place < first_hub + H)
    side = jnp.where(place >= G // 2, 1, 0)
    lane_of = bits_of(place, G)[-1][1] if per_k == 2 else lax.rem(place, per_k)

    def hub(r, c):
        return r * G + first_hub + c

    barrier = pltpu.get_barrier_semaphore()
    for d in range(1, S):
        pl.semaphore_signal(
            barrier, inc=1, device_id={"seq": peers[d]}, device_id_type=MESH
        )
    for d in range(1, T):
        pl.semaphore_signal(
            barrier, inc=1, device_id={"tp": twins[d]}, device_id_type=MESH
        )

    loads = []
    for i, (src, dst) in enumerate(
        (
            (q_hbm, q_ref),
            (k_hbm, k_ref),
            (v_hbm, v_ref),
            (lens_hbm, lens_ref),
            (ck_hbm, ck),
            (cv_hbm, cv),
            (anc_hbm, anc_ref),
            (ow_hbm, ow),
            (rk_hbm, rk),
            (rv_hbm, rv),
            (ridx_hbm, ridx_ref),
            (hid_hbm, hid_ref),
            (gain_hbm, gain_ref),
        )
    ):
        copy = pltpu.make_async_copy(src, dst, load_sem.at[i])
        copy.start()
        loads.append(copy)
    for c in range(H):
        source, at = (wk_hbm, c) if c < H // 2 else (wv_hbm, c - H // 2)
        for src, dst in (
                (wq_hbm.at[:, pl.ds(c * qcols, qcols)], weight.at[c, :, pl.ds(0, qcols)]),
                (source.at[:, pl.ds(at * kcols, kcols)], weight.at[c, :, pl.ds(qcols, kcols)]),
        ):
            pltpu.make_async_copy(src, dst, weight_sem).start()

    def remote(phase, src, dst, at, target):
        return pltpu.make_async_remote_copy(
            src_ref=src,
            dst_ref=dst,
            send_sem=send_sem.at[phase],
            recv_sem=recv_sem.at[at],
            device_id={"seq": target},
            device_id_type=MESH,
        )

    def send(phase, src, dst, at, target, when=None):
        copy = remote(phase, src, dst, at, target)
        if when is None:
            copy.start()
        else:
            pl.when(when)(copy.start)

    def send_twin(phase, src, dst, at, target):
        pltpu.make_async_remote_copy(
            src_ref=src,
            dst_ref=dst,
            send_sem=send_sem.at[phase],
            recv_sem=recv_sem.at[at],
            device_id={"tp": target},
            device_id_type=MESH,
        ).start()

    def arrive(at, block, when=None):
        copy = remote(0, block, block, at, peers[1])
        if when is None:
            copy.wait_recv()
        else:
            pl.when(when)(copy.wait_recv)

    def gone(phase, block, when=None):
        copy = remote(phase, block, block, 0, peers[1])
        if when is None:
            copy.wait_send()
        else:
            pl.when(when)(copy.wait_send)

    at_heads = 8
    at_upper = at_heads + R * H

    row_a = lax.broadcasted_iota(jnp.int32, (lanes, lanes), 0)
    col_a = lax.broadcasted_iota(jnp.int32, (lanes, lanes), 1)

    def one_hot(where):
        return jnp.where(where, 1.0, 0.0).astype(BF16)

    form[kv] = jnp.zeros(form.shape[1:], F32)
    for i in range(3):
        loads[i].wait()
    q_rows = q_ref[...].astype(F32)
    k_rows = k_ref[...].astype(F32)
    v_rows = v_ref[...].astype(F32)
    for k in range(kv):
        for j in range(g):
            h = k * g + j
            form[k, pl.ds(j, own, stride=g), :] = q_rows[:, h * hd : (h + 1) * hd]
        form[kv, pl.ds(k, own, stride=g), :] = k_rows[:, k * hd : (k + 1) * hd]
        form[kv, pl.ds(kv + k, own, stride=g), :] = v_rows[:, k * hd : (k + 1) * hd]
    for k in range(kv + 1):
        low[me, k] = form[k, :rows, :].astype(BF16)

    pl.semaphore_wait(barrier, S - 1 + T - 1)

    for d in reversed(range(1, S)):
        own_q = low.at[me, pl.ds(0, kv)]
        send(0, own_q, own_q, 0, peers[d])
    for c in range(H):
        own_kv = low.at[me, pl.ds(kv, 1)]
        target = hub(request, c)
        send(1, own_kv, own_kv, 1, target, target != me)

    for i in range(3, 7):
        loads[i].wait()
    columns = ckeys.shape[2]
    first = me * columns
    position = lax.broadcasted_iota(jnp.int32, (columns, hd), 0) + first
    for r in range(R):
        wide[: columns * kv] = ck[r].astype(F32)
        allowed = jnp.where(position < lens_ref[r], 0.0, masked_score).astype(BF16)
        for k in range(kv):
            ckeys[r, k, :, :hd] = wide[pl.ds(k, columns, stride=kv), :].astype(BF16)
            ckeys[r, k, :, hd:] = allowed
        wide[: columns * kv] = cv[r].astype(F32)
        for k in range(kv):
            cvals[r, k, :hd, :] = wide[pl.ds(k, columns, stride=kv), :].T.astype(BF16)
            cvals[r, k, hd:, :] = jnp.ones((cvals.shape[2] - hd, columns), BF16)

    lead = one_hot(lax.broadcasted_iota(jnp.int32, (lanes, hd), 1) == 0)
    row_s = lax.broadcasted_iota(jnp.int32, (16, lanes), 0)
    arrive(0, low.at[pl.ds(0, S - 1), pl.ds(0, kv)])

    for r in range(R):
        for step in range(kv):
            k = turn(side, kv - 1 - step, kv)
            queries = low[pl.ds(r * G, G), k].reshape(lanes, hd)
            queries = jnp.concatenate([queries, lead], axis=1)
            scores = contract_last(ckeys[r, k], queries)
            high = jnp.maximum(jnp.max(scores, axis=0, keepdims=True), lowest_high)
            high = high.astype(BF16).astype(F32)
            mass = jnp.exp2((scores - high) * sharp).astype(BF16)
            blend = jnp.dot(cvals[r, k], mass, preferred_element_type=F32)
            total = blend[hd : hd + 1]
            coarse = total.astype(BF16).astype(F32)
            stats = jnp.where(row_s == 1, coarse, jnp.where(row_s == 2, total - coarse, 0.0))
            stats = jnp.where(row_s == 0, high, stats).astype(BF16)
            for h in range(per_k):
                at = r * H + k * per_k + h
                part[at, :slab, :] = blend[h * slab : (h + 1) * slab].astype(BF16)
                part[at, slab:, :] = stats
            for d in reversed(range(per_k)):
                c = k * per_k + turn(lane_of, d, per_k)
                target = hub(r, c)
                send(2, part.at[r * H + c], gpart.at[me], 2, target, target != me)

    @pl.when(is_hub)
    def _():
        k = jnp.where(slot >= per_k, 1, 0) if kv == 2 else lax.div(slot, per_k)
        part_of = slot - k * per_k
        ancestry = anc_ref[request].astype(F32).astype(BF16)
        spread = one_hot(
            lax.div(lax.broadcasted_iota(jnp.int32, (lanes, nodes), 0), g)
            == lax.broadcasted_iota(jnp.int32, (lanes, nodes), 1)
        )
        mask = jnp.dot(spread, ancestry, preferred_element_type=F32).astype(BF16)
        small = one_hot(
            lax.broadcasted_iota(jnp.int32, (nodes, nodes), 0)
            == lax.broadcasted_iota(jnp.int32, (nodes, nodes), 1)
        )
        mask = contract_last(small, mask)
        arrive(1, low.at[pl.ds(0, G - 1), pl.ds(kv, 1)])
        form[kv, :lanes, :] = low[pl.ds(base, G), kv].reshape(lanes, hd).astype(F32)
        keys = form[kv, pl.ds(k, nodes, stride=g), :].astype(BF16)
        values = form[kv, pl.ds(kv + k, nodes, stride=g), :].astype(BF16)
        scores = contract_last(keys, low[pl.ds(base, G), k].reshape(lanes, hd))
        scores = jnp.where(mask > 0.5, scores, masked_score)
        near_high = jnp.max(scores, axis=0, keepdims=True)
        mass = jnp.exp2((scores - near_high) * sharp)
        near_total = jnp.sum(mass, axis=0, keepdims=True)
        turned = contract_last(one_hot(row_a == col_a)[:hd, :hd], values).astype(BF16)
        wide[:hd] = jnp.dot(turned, mass.astype(BF16), preferred_element_type=F32)
        near = wide[pl.ds(pl.multiple_of(part_of * slab, slab), slab), :]
        gpart[me] = part[request * H + slot]
        arrive(2, gpart.at[pl.ds(0, S - 1)])
        for s in range(S):
            tops[s * 16 : (s + 1) * 16] = gpart[s, slab:].astype(F32)
        highs = tops[pl.ds(0, S, stride=16), :]
        totals = tops[pl.ds(1, S, stride=16), :] + tops[pl.ds(2, S, stride=16), :]
        top = jnp.maximum(jnp.max(highs, axis=0, keepdims=True), near_high)
        factors = jnp.exp2((highs - top) * sharp)
        late = jnp.exp2((near_high - top) * sharp)
        total = jnp.sum(factors * totals, axis=0, keepdims=True) + near_total * late
        acc = near * late
        for s in range(S):
            acc = acc + gpart[s, :slab].astype(F32) * factors[s : s + 1]
        heads[request * H + slot] = (acc * (1.0 / total)).astype(BF16)

    for d in reversed(range(1, S)):
        done = heads.at[request * H + slot]
        send(3, done, done, at_heads + request * H + slot, peers[d], is_hub)

    entries = rkeys.shape[1]
    for i in range(7, 11):
        loads[i].wait()
    wide[: entries * kv] = rk[...].astype(F32)
    for k in range(kv):
        rkeys[k] = wide[pl.ds(k, entries, stride=kv), :].astype(BF16)
    wide[: entries * kv] = rv[...].astype(F32)
    for k in range(kv):
        rvals[k, :, :hd] = wide[pl.ds(k, entries, stride=kv), :].astype(BF16)
        rvals[k, :, hd:] = jnp.ones((entries, hd), BF16)
        kept = jnp.where(ridx_ref[k : k + 1, :] < lens_ref[request], 0.0, masked_score)
        bias_ref[k] = jnp.broadcast_to(kept, bias_ref.shape[1:])
    mask_rows = []
    for r in range(own):
        row = anc_ref[request, pl.ds(place * own + r, 1), :]
        mask_rows.append(jnp.broadcast_to(row, (g, nodes)))
    tree_mask = jnp.concatenate(mask_rows, axis=0) > 0
    order = one_hot(
        jnp.logical_and(
            lax.rem(row_a, nodes) == lax.div(col_a, g),
            lax.div(row_a, nodes) == lax.rem(col_a, g),
        )
    )

    summed = None
    for step in range(kv):
        k = turn(side, step, kv)
        lower = []
        for r in range(R):
            for d in range(per_k):
                c = k * per_k + turn(lane_of, d, per_k)
                at = r * H + c
                arrive(at_heads + at, heads.at[at], hub(r, c) != me)
            turned = heads[pl.ds(r * H + k * per_k, per_k)].reshape(hd, lanes)
            turned = contract_last(order, turned).astype(BF16)
            lower.append(
                jnp.concatenate(
                    [turned[j * nodes : (j + 1) * nodes] for j in range(g)], axis=1
                )
            )
        lower = lower[0] if R == 1 else jnp.concatenate(lower, axis=0)
        depth = g * hd
        start = pl.multiple_of(k * depth, depth)
        if step < kv - 1:
            more = jnp.dot(lower, ow[pl.ds(start, depth), :], preferred_element_type=F32)
            summed = more if summed is None else summed + more
        else:
            for p in range(2):
                more = jnp.dot(
                    lower,
                    ow[pl.ds(start, depth), p * half : (p + 1) * half],
                    preferred_element_type=F32,
                )
                if summed is not None:
                    more = more + summed[:, p * half : (p + 1) * half]
                terms[tp, p] = more.astype(BF16)
                for d in reversed(range(1, T)):
                    mine = terms.at[tp, p]
                    send_twin(4, mine, mine, 3 + p, twins[d])
    loads[11].wait()
    loads[12].wait()
    residual = []
    for p in range(2):
        arrive(3 + p, terms.at[pl.ds(0, T - 1), p])
        summed = terms[0, p].astype(F32)
        for t in range(1, T):
            summed = summed + terms[t, p].astype(F32)
        residual.append(hid_ref[:, p * half : (p + 1) * half].astype(F32) + summed)
    residual = jnp.concatenate(residual, axis=1)

    squares = jnp.broadcast_to(jnp.sum(residual * residual, axis=1, keepdims=True), (M, hd))
    coarse = squares.astype(BF16).astype(F32)
    lane = lax.broadcasted_iota(jnp.int32, (M, hd), 1)
    squares = jnp.where(lane < hd // 2, coarse, squares - coarse).astype(BF16)
    for r in range(R):
        square[r] = squares[r * nodes : (r + 1) * nodes]
        for c in range(H):
            target = hub(r, c)
            send(5, square.at[r], gsquare.at[me], 5, target, target != me)
    pltpu.make_async_copy(weight, weight, weight_sem).wait()
    scaled = (residual * gain_ref[...]).astype(BF16)
    for step in range(kv):
        for d in reversed(range(per_k)):
            c = turn(side, kv - 1 - step, kv) * per_k + turn(lane_of, d, per_k)
            out = jnp.dot(scaled, weight[c], preferred_element_type=F32).astype(BF16)
            for r in range(R):
                proj[r * H + c] = out[r * nodes : (r + 1) * nodes]
                target = hub(r, c)
                send(6, proj.at[r * H + c], gproj.at[me], 6, target, target != me)
    res_ref[...] = residual

    @pl.when(is_hub)
    def _():
        gsquare[me] = square[request]
        gproj[me] = proj[request * H + slot]
        arrive(5, gsquare.at[pl.ds(0, S - 1)])
        total = gsquare[0].astype(F32)
        for s in range(1, S):
            total = total + gsquare[s].astype(F32)
        total = total + pltpu.roll(total, hd // 2, 1)
        inverse = lax.rsqrt(total / width + norm_epsilon)
        arrive(6, gproj.at[pl.ds(0, S - 1)])
        for t in range((qcols + kcols) // hd):
            at = slice(t * hd, (t + 1) * hd)
            total = gproj[0, :, at].astype(F32)
            for s in range(1, S):
                total = total + gproj[s, :, at].astype(F32)
            upper[slot, :, at] = (total * inverse).astype(BF16)

    for d in reversed(range(1, G)):
        mine = upper.at[slot]
        send(7, mine, mine, at_upper + slot, base + mates[d], is_hub)

    spot = lax.broadcasted_iota(jnp.int32, (lanes, hd), 1)
    third = hd // 4

    def pack_stats(high, total):
        packed = jnp.where(jnp.bitwise_and(spot, 1) == 0, high, total)
        coarse = packed.astype(BF16).astype(F32)
        rest = packed - coarse
        middle = rest.astype(BF16).astype(F32)
        fine = rest - middle
        packed = jnp.where(spot < third, coarse, jnp.where(spot < 2 * third, middle, fine))
        return jnp.where(spot < 3 * third, packed, 0.0)

    def unpack_stats(block):
        packed = block.astype(F32)
        return (packed + pltpu.roll(packed, hd - third, 1)) + pltpu.roll(
            packed, hd - 2 * third, 1
        )

    pick = one_hot(
        jnp.logical_and(
            lax.div(lax.broadcasted_iota(jnp.int32, (rows, lanes), 0), g) + place * own
            == lax.rem(lax.broadcasted_iota(jnp.int32, (rows, lanes), 1), nodes),
            lax.rem(lax.broadcasted_iota(jnp.int32, (rows, lanes), 0), g)
            == lax.div(lax.broadcasted_iota(jnp.int32, (rows, lanes), 1), nodes),
        )
    )

    def upper_queries(k):
        tiles = []
        for j in range(g):
            tile = upper[k * per_k + j // hub_heads]
            tiles.append(tile[:, (j % hub_heads) * hd : (j % hub_heads + 1) * hd])
        return jnp.concatenate(tiles, axis=0)

    for step in range(kv):
        k = turn(side, step, kv)
        for d in range(per_k):
            c = k * per_k + turn(lane_of, d, per_k)
            arrive(at_upper + c, upper.at[c], hub(request, c) != me)
        scores = contract_last(upper_queries(k), rkeys[k]) + bias_ref[k, 0:1, :]
        high = jnp.maximum(jnp.max(scores, axis=1, keepdims=True), lowest_high)
        mass = jnp.exp2((scores - high) * sharp).astype(BF16)
        blend = jnp.dot(mass, rvals[k], preferred_element_type=F32)
        form[0, :lanes, :] = blend[:, :hd]
        form[1, :lanes, :] = pack_stats(high, blend[:, hd:])
        for a in range(G):
            for i in range(2):
                tile = [form[i, pl.ds(a * own + b, g, stride=nodes), :] for b in range(own)]
                upart[a, k, i * rows : (i + 1) * rows, :] = jnp.concatenate(tile, axis=0).astype(
                    BF16
                )
        for d in reversed(range(1, G)):
            target = mates[d]
            send(8, upart.at[target, k], ugpart.at[place, k], 7, base + target)
    ugpart[place] = upart[place]

    trees = []
    for k in range(kv):
        queries = jnp.dot(pick, upper_queries(k), preferred_element_type=F32).astype(BF16)
        keys = upper[(k * hd) // kcols][:, qcols:]
        values = upper[H // 2 + (k * hd) // kcols][:, qcols:]
        scores = jnp.where(tree_mask, contract_last(queries, keys), masked_score)
        high = jnp.max(scores, axis=1, keepdims=True)
        mass = jnp.exp2((scores - high) * sharp)
        total = jnp.sum(mass, axis=1, keepdims=True)
        trees.append((jnp.dot(mass.astype(BF16), values, preferred_element_type=F32), high, total))
    arrive(7, ugpart.at[pl.ds(0, G - 1)])
    for k in range(kv):
        blend, high, total = trees[k]
        stats = [unpack_stats(ugpart[s, k, rows:]) for s in range(G)]
        top = jnp.maximum(functools.reduce(jnp.maximum, stats)[:, 0:1], high)
        late = jnp.exp2((high - top) * sharp)
        acc = blend * late
        whole = total * late
        mass = jnp.zeros((rows, hd), F32)
        for s in range(G):
            factor = jnp.exp2((stats[s] - top) * sharp)
            acc = acc + ugpart[s, k, :rows].astype(F32) * factor[:, 0:1]
            mass = mass + pltpu.roll(stats[s], hd - 1, 1) * factor
        form[k, :rows, :] = acc / (whole + mass[:, 0:1])
        for j in range(g):
            h = k * g + j
            up_ref[:, h * hd : (h + 1) * hd] = form[k, pl.ds(j, own, stride=g), :]
    far = jnp.logical_not(is_hub)
    gone(0, low.at[pl.ds(0, S - 1), pl.ds(0, kv)])
    gone(1, low.at[pl.ds(0, H), pl.ds(kv, 1)], far)
    gone(1, low.at[pl.ds(0, H - 1), pl.ds(kv, 1)], is_hub)
    gone(2, part.at[pl.ds(0, R * H)], far)
    gone(2, part.at[pl.ds(0, R * H - 1)], is_hub)
    gone(3, heads.at[pl.ds(0, S - 1)], is_hub)
    gone(4, terms.at[pl.ds(0, T - 1)])
    gone(5, gsquare.at[pl.ds(0, R * H)], far)
    gone(5, gsquare.at[pl.ds(0, R * H - 1)], is_hub)
    gone(6, proj.at[pl.ds(0, R * H)], far)
    gone(6, proj.at[pl.ds(0, R * H - 1)], is_hub)
    gone(7, upper.at[pl.ds(0, G - 1)], is_hub)
    gone(8, upart.at[pl.ds(0, G - 1)])


def shards(
    tree_hidden,
    query_low,
    key_tree_low,
    value_tree_low,
    cache_keys,
    cache_values,
    cache_lengths,
    ancestors,
    out_weight,
    norm_gain,
    w_query_up,
    w_key_up,
    w_value_up,
    retained_keys,
    retained_values,
    retained_index,
):
    S = lax.axis_size("seq")
    T = lax.axis_size("tp")
    R, part, kv, hd = cache_keys.shape
    own, row_width = query_low.shape
    g = row_width // (kv * hd)
    G = S // R
    M = S * own
    rows = own * g
    features = tree_hidden.shape[1]
    entries = retained_keys.shape[1] * kv
    ck = cache_keys.reshape(R, part * kv, hd)
    cv = cache_values.reshape(R, part * kv, hd)
    rk = retained_keys.reshape(entries, hd)
    rv = retained_values.reshape(entries, hd)
    ridx = retained_index[0].T
    gain = norm_gain.reshape(1, features)
    vmem = pl.BlockSpec(memory_space=pltpu.VMEM)
    hbm = pl.BlockSpec(memory_space=pl.ANY)
    H = G // 2
    columns = part
    big = (
        query_low,
        key_tree_low,
        value_tree_low,
        ck,
        cv,
        ancestors,
        out_weight,
        tree_hidden,
        gain,
        ridx,
        rk,
        rv,
    )
    cols = (kv * g * hd + 2 * kv * hd) // H
    nodes = G * own
    lanes = nodes * g
    slab = hd * kv // H
    outs = pl.pallas_call(
        functools.partial(kernel, (S, T, R, own, kv, g, hd)),
        out_shape=(
            pltpu.VMEM((M, features), F32),
            pltpu.VMEM((own, row_width), F32),
        ),
        in_specs=[hbm] * (4 + len(big)),
        out_specs=(vmem, vmem),
        scratch_shapes=[pltpu.SMEM((R,), jnp.int32)]
        + [pltpu.VMEM(x.shape, x.dtype) for x in big]
        + [
            pltpu.VMEM((H, features, cols), BF16),
            pltpu.VMEM((kv + 1, lanes, hd), F32),
            pltpu.VMEM((max(columns * kv, entries), hd), F32),
            pltpu.VMEM((R, kv, columns, 2 * hd), BF16),
            pltpu.VMEM((R, kv, hd + 16, columns), BF16),
            pltpu.VMEM((kv, entries // kv, hd), BF16),
            pltpu.VMEM((kv, entries // kv, 2 * hd), BF16),
            pltpu.VMEM((kv, 8, entries // kv), F32),
            pltpu.VMEM((S, kv + 1, rows, hd), BF16),
            pltpu.VMEM((R * H, slab + 16, lanes), BF16),
            pltpu.VMEM((S, slab + 16, lanes), BF16),
            pltpu.VMEM((S * 16, lanes), F32),
            pltpu.VMEM((S, slab, lanes), BF16),
            pltpu.VMEM((T, 2, M, features // 2), BF16),
            pltpu.VMEM((R * H, nodes, cols), BF16),
            pltpu.VMEM((S, nodes, cols), BF16),
            pltpu.VMEM((R, nodes, hd), BF16),
            pltpu.VMEM((S, nodes, hd), BF16),
            pltpu.VMEM((G, nodes, cols), BF16),
            pltpu.VMEM((G, kv, 2 * rows, hd), BF16),
            pltpu.VMEM((G, kv, 2 * rows, hd), BF16),
            pltpu.SemaphoreType.DMA((1 + len(big),)),
            pltpu.SemaphoreType.DMA,
            pltpu.SemaphoreType.DMA((9,)),
            pltpu.SemaphoreType.DMA((8 + R * H + H,)),
        ],
        compiler_params=pltpu.CompilerParams(
            collective_id=0, has_side_effects=True, vmem_limit_bytes=56 * 1024 * 1024
        ),
        name="two_layers",
    )(
        cache_lengths,
        *big,
        w_key_up,
        w_value_up,
        w_query_up,
    )

    def settle(a_ref, b_ref, c_ref, d_ref):
        c_ref[...] = a_ref[...]
        d_ref[...] = b_ref[...]

    return pl.pallas_call(
        settle,
        out_shape=tuple(jax.ShapeDtypeStruct(x.shape, x.dtype) for x in outs),
        in_specs=[vmem] * 2,
        out_specs=(vmem, vmem),
        name="settle",
    )(*[pltpu.with_memory_space_constraint(x, pltpu.VMEM) for x in outs])


def solution(mesh):
    return jax.shard_map(
        shards,
        mesh=mesh,
        in_specs=(
            P(None, "seq"),
            P("seq", "tp"),
            P("seq", "tp"),
            P("seq", "tp"),
            P(None, "seq", "tp", None),
            P(None, "seq", "tp", None),
            P(),
            P(),
            P("tp", "seq"),
            P("seq"),
            P("seq", "tp"),
            P("seq", "tp"),
            P("seq", "tp"),
            P("seq", None, "tp", None),
            P("seq", None, "tp", None),
            P("seq", None, "tp"),
        ),
        out_specs=(P(None, "seq"), P("seq", "tp")),
        check_vma=False,
    )
```

```python
import functools
import math

import jax
import jax.numpy as jnp
from jax import lax
from jax.experimental import pallas as pl
from jax.experimental.pallas import tpu as pltpu
from jax.sharding import PartitionSpec as P

MESH = pl.DeviceIdType.MESH
F32 = jnp.float32
BF16 = jnp.bfloat16
masked_score = -1e30
lowest_high = -1e29
norm_epsilon = 1e-05
last_last = (((1,), (1,)), ((), ()))


def contract_last(a, b):
    return lax.dot_general(a, b, last_last, preferred_element_type=F32)


def bits_of(index, count):
    found = []
    bit = 1
    while 2 * bit < count:
        bit *= 2
    while bit and count > 1:
        there = jnp.where(index >= bit, 1, 0)
        index = index - there * bit
        found.append((bit, there))
        bit //= 2
    return found


def flips(index, count):
    steps = [(bit, (1 - 2 * there) * bit) for bit, there in bits_of(index, count)]
    result = []
    for d in range(count):
        other = index
        for bit, step in steps:
            if d & bit:
                other = other + step
        result.append(other)
    return result


def turn(index, step, count):
    if step % count == 0:
        return index
    if count == 2:
        return 1 - index
    return lax.rem(index + step, count)


def kernel(
    sizes,
    lens_hbm,
    q_hbm,
    k_hbm,
    v_hbm,
    ck_hbm,
    cv_hbm,
    anc_hbm,
    ow_hbm,
    hid_hbm,
    gain_hbm,
    ridx_hbm,
    rk_hbm,
    rv_hbm,
    wk_hbm,
    wv_hbm,
    wq_hbm,
    res_ref,
    up_ref,
    lens_ref,
    anc_ref,
    ow,
    hid_ref,
    gain_ref,
    ridx_ref,
    mine,
    cache,
    kept_rows,
    weight,
    near_weight,
    form,
    wide,
    ckeys,
    cvals,
    rkeys,
    rvals,
    bias_ref,
    low,
    part,
    gpart,
    tops,
    heads,
    terms,
    proj,
    gproj,
    near_proj,
    near_gproj,
    square,
    gsquare,
    upper,
    near_upper,
    inverse_ref,
    upart,
    ugpart,
    load_sem,
    send_sem,
    recv_sem,
):
    S, T, R, own, kv, g, hd = sizes
    G = S // R
    H = G // 2
    M = S * own
    rows = own * g
    nodes = G * own
    lanes = nodes * g
    per_k = H // kv
    slab = hd // per_k
    qcols = kv * g * hd // H
    kcols = 2 * kv * hd // H
    hub_heads = qcols // hd
    scale = hd ** (-0.5)
    sharp = scale * math.log2(math.e)
    width = S * hid_ref.shape[1]
    pieces = terms.shape[1]
    piece = hid_ref.shape[1] // pieces
    me = lax.axis_index("seq")
    tp = lax.axis_index("tp")
    request = 0 if R == 1 else lax.div(me, G)
    base = request * G
    place = me - base
    peers = flips(me, S)
    mates = flips(place, G)
    twins = flips(tp, T)
    first_hub = G // 4
    slot = place - first_hub
    is_hub = jnp.logical_and(place >= first_hub, place < first_hub + H)
    side = jnp.where(place >= G // 2, 1, 0)
    lane_of = bits_of(place, G)[-1][1] if per_k == 2 else lax.rem(place, per_k)

    def hub(r, c):
        return r * G + first_hub + c

    barrier = pltpu.get_barrier_semaphore()
    for d in reversed(range(1, S)):
        pl.semaphore_signal(
            barrier, inc=1, device_id={"seq": peers[d]}, device_id_type=MESH
        )
    for d in range(1, T):
        pl.semaphore_signal(
            barrier, inc=1, device_id={"tp": twins[d]}, device_id_type=MESH
        )

    row_width = kv * g * hd
    features = hid_ref.shape[1]
    depth = cache.shape[0] // (2 * R)
    ready = {}
    for i, (name, pairs, whole) in enumerate(
        (
            (
                "mine",
                (
                    (q_hbm, mine.at[:, pl.ds(0, row_width)]),
                    (k_hbm, mine.at[:, pl.ds(row_width, kv * hd)]),
                    (v_hbm, mine.at[:, pl.ds(row_width + kv * hd, kv * hd)]),
                ),
                mine,
            ),
            ("length", ((lens_hbm, lens_ref),), lens_ref),
            (
                "cache",
                (
                    (ck_hbm, cache.at[pl.ds(0, R * depth)]),
                    (cv_hbm, cache.at[pl.ds(R * depth, R * depth)]),
                ),
                cache,
            ),
            ("tree", ((anc_hbm, anc_ref),), anc_ref),
            ("out", ((ow_hbm, ow),), ow),
            ("kept", ((rk_hbm, kept_rows.at[0]), (rv_hbm, kept_rows.at[1])), kept_rows),
            ("index", ((ridx_hbm, ridx_ref),), ridx_ref),
            ("hidden", ((hid_hbm, hid_ref),), hid_ref),
            ("gain", ((gain_hbm, gain_ref),), gain_ref),
            (
                "query",
                [(wq_hbm.at[:, pl.ds(c * qcols, qcols)], weight.at[c]) for c in range(H)],
                weight,
            ),
            (
                "near",
                (
                    (wk_hbm, near_weight.at[:, pl.ds(0, kv * hd)]),
                    (wv_hbm, near_weight.at[:, pl.ds(kv * hd, kv * hd)]),
                ),
                near_weight,
            ),
        )
    ):
        for source, there in pairs:
            pltpu.make_async_copy(source, there, load_sem.at[i]).start()
        ready[name] = pltpu.make_async_copy(whole, whole, load_sem.at[i])

    def remote(src, dst, at, target):
        return pltpu.make_async_remote_copy(
            src_ref=src,
            dst_ref=dst,
            send_sem=send_sem,
            recv_sem=recv_sem.at[at],
            device_id={"seq": target},
            device_id_type=MESH,
        )

    def send(src, dst, at, target, when=None):
        copy = remote(src, dst, at, target)
        if when is None:
            copy.start()
        else:
            pl.when(when)(copy.start)

    def send_twin(src, dst, at, target):
        pltpu.make_async_remote_copy(
            src_ref=src,
            dst_ref=dst,
            send_sem=send_sem,
            recv_sem=recv_sem.at[at],
            device_id={"tp": target},
            device_id_type=MESH,
        ).start()

    def arrive(at, block, when=None):
        copy = remote(block, block, at, peers[1])
        if when is None:
            copy.wait_recv()
        else:
            pl.when(when)(copy.wait_recv)

    at_heads = 8
    at_upper = at_heads + kv
    at_terms = at_upper + kv
    own_k = jnp.where(slot >= per_k, 1, 0) if kv == 2 else lax.div(slot, per_k)

    row_a = lax.broadcasted_iota(jnp.int32, (lanes, lanes), 0)
    col_a = lax.broadcasted_iota(jnp.int32, (lanes, lanes), 1)

    def one_hot(where):
        return jnp.where(where, 1.0, 0.0).astype(BF16)

    form[kv] = jnp.zeros(form.shape[1:], F32)
    ready["mine"].wait()
    all_rows = mine[...].astype(F32)
    q_rows = all_rows[:, :row_width]
    k_rows = all_rows[:, row_width : row_width + kv * hd]
    v_rows = all_rows[:, row_width + kv * hd :]
    for k in range(kv):
        for j in range(g):
            h = k * g + j
            form[k, pl.ds(j, own, stride=g), :] = q_rows[:, h * hd : (h + 1) * hd]
        form[kv, pl.ds(k, own, stride=g), :] = k_rows[:, k * hd : (k + 1) * hd]
        form[kv, pl.ds(kv + k, own, stride=g), :] = v_rows[:, k * hd : (k + 1) * hd]
    for k in range(kv + 1):
        low[me, k] = form[k, :rows, :].astype(BF16)

    pl.semaphore_wait(barrier, S - 1 + T - 1)

    for d in reversed(range(1, S)):
        own_q = low.at[me, pl.ds(0, kv)]
        send(own_q, own_q, 0, peers[d])
    for c in range(H):
        own_kv = low.at[me, pl.ds(kv, 1)]
        target = hub(request, c)
        send(own_kv, own_kv, 1, target, target != me)

    for name in ("length", "cache", "tree"):
        ready[name].wait()
    columns = cvals.shape[3]
    first = me * columns
    position = lax.broadcasted_iota(jnp.int32, (columns, hd), 0) + first
    for r in range(R):
        wide[: columns * kv] = cache[r * depth : (r + 1) * depth].astype(F32)
        allowed = jnp.where(position < lens_ref[r], 0.0, masked_score).astype(BF16)
        for k in range(kv):
            at = pl.ds((r * kv + k) * columns, columns)
            ckeys[at, :hd] = wide[pl.ds(k, columns, stride=kv), :].astype(BF16)
            ckeys[at, hd:] = allowed
        wide[: columns * kv] = cache[(R + r) * depth : (R + r + 1) * depth].astype(F32)
        for k in range(kv):
            cvals[r, k, :hd, :] = wide[pl.ds(k, columns, stride=kv), :].T.astype(BF16)
            cvals[r, k, hd:, :] = jnp.ones((cvals.shape[2] - hd, columns), BF16)

    lead = one_hot(lax.broadcasted_iota(jnp.int32, (lanes, hd), 1) == 0)
    row_s = lax.broadcasted_iota(jnp.int32, (8, lanes), 0)
    arrive(0, low.at[pl.ds(0, S - 1), pl.ds(0, kv)])

    for r in range(R):
        for step in range(kv):
            k = turn(side, kv - 1 - step, kv)
            queries = low[pl.ds(r * G, G), k].reshape(lanes, hd)
            queries = jnp.concatenate([queries, lead], axis=1)
            cut = columns // 4
            start = pl.multiple_of((r * kv + k) * columns, columns)
            scores = [
                contract_last(ckeys[pl.ds(start + p * cut, cut), :], queries) for p in range(4)
            ]
            high = functools.reduce(
                jnp.maximum, [jnp.max(x, axis=0, keepdims=True) for x in scores]
            )
            high = jnp.maximum(high, lowest_high).astype(BF16).astype(F32)
            blend = sum(
                jnp.dot(
                    cvals[r, k, :, p * cut : (p + 1) * cut],
                    jnp.exp2((x - high) * sharp).astype(BF16),
                    preferred_element_type=F32,
                )
                for p, x in enumerate(scores)
            )
            total = blend[hd : hd + 1]
            coarse = total.astype(BF16).astype(F32)
            stats = jnp.where(row_s == 1, coarse, jnp.where(row_s == 2, total - coarse, 0.0))
            stats = jnp.where(row_s == 0, high, stats).astype(BF16)
            for h in range(per_k):
                at = r * H + k * per_k + h
                part[at, :slab, :] = blend[h * slab : (h + 1) * slab].astype(BF16)
                part[at, slab:, :] = stats
            for d in reversed(range(per_k)):
                c = k * per_k + turn(lane_of, d, per_k)
                target = hub(r, c)
                send(part.at[r * H + c], gpart.at[me], 2, target, target != me)

    @pl.when(is_hub)
    def _():
        k = jnp.where(slot >= per_k, 1, 0) if kv == 2 else lax.div(slot, per_k)
        part_of = slot - k * per_k
        ancestry = anc_ref[request].astype(F32).astype(BF16)
        spread = one_hot(
            lax.div(lax.broadcasted_iota(jnp.int32, (lanes, nodes), 0), g)
            == lax.broadcasted_iota(jnp.int32, (lanes, nodes), 1)
        )
        mask = jnp.dot(spread, ancestry, preferred_element_type=F32).astype(BF16)
        small = one_hot(
            lax.broadcasted_iota(jnp.int32, (nodes, nodes), 0)
            == lax.broadcasted_iota(jnp.int32, (nodes, nodes), 1)
        )
        mask = contract_last(small, mask)
        arrive(1, low.at[pl.ds(0, G - 1), pl.ds(kv, 1)])
        form[kv, :lanes, :] = low[pl.ds(base, G), kv].reshape(lanes, hd).astype(F32)
        keys = form[kv, pl.ds(k, nodes, stride=g), :].astype(BF16)
        values = form[kv, pl.ds(kv + k, nodes, stride=g), :].astype(BF16)
        scores = contract_last(keys, low[pl.ds(base, G), k].reshape(lanes, hd))
        scores = jnp.where(mask > 0.5, scores, masked_score)
        near_high = jnp.max(scores, axis=0, keepdims=True)
        mass = jnp.exp2((scores - near_high) * sharp)
        near_total = jnp.sum(mass, axis=0, keepdims=True)
        turned = contract_last(one_hot(row_a == col_a)[:hd, :hd], values).astype(BF16)
        wide[:hd] = jnp.dot(turned, mass.astype(BF16), preferred_element_type=F32)
        near = wide[pl.ds(pl.multiple_of(part_of * slab, slab), slab), :]
        gpart[me] = part[request * H + slot]
        arrive(2, gpart.at[pl.ds(0, S - 1)])
        for s in range(S):
            tops[s * 8 : (s + 1) * 8] = gpart[s, slab:].astype(F32)
        highs = tops[pl.ds(0, S, stride=8), :]
        totals = tops[pl.ds(1, S, stride=8), :] + tops[pl.ds(2, S, stride=8), :]
        top = jnp.maximum(jnp.max(highs, axis=0, keepdims=True), near_high)
        factors = jnp.exp2((highs - top) * sharp)
        late = jnp.exp2((near_high - top) * sharp)
        total = jnp.sum(factors * totals, axis=0, keepdims=True) + near_total * late
        acc = near * late
        for s in range(S):
            acc = acc + gpart[s, :slab].astype(F32) * factors[s : s + 1]
        heads[request * H + slot] = (acc * (1.0 / total)).astype(BF16)

    for d in reversed(range(1, S)):
        done = heads.at[request * H + slot]
        send(done, done, at_heads + own_k, peers[d], is_hub)

    entries = rkeys.shape[1]
    for name in ("out", "kept", "index"):
        ready[name].wait()
    wide[: entries * kv] = kept_rows[0].astype(F32)
    for k in range(kv):
        rkeys[k] = wide[pl.ds(k, entries, stride=kv), :].astype(BF16)
    wide[: entries * kv] = kept_rows[1].astype(F32)
    for k in range(kv):
        rvals[k, :, :hd] = wide[pl.ds(k, entries, stride=kv), :].astype(BF16)
        rvals[k, :, hd:] = jnp.ones((entries, hd), BF16)
        kept = jnp.where(ridx_ref[k : k + 1, :] < lens_ref[request], 0.0, masked_score)
        bias_ref[k] = jnp.broadcast_to(kept, bias_ref.shape[1:])
    mask_rows = []
    for r in range(own):
        row = anc_ref[request, pl.ds(place * own + r, 1), :]
        mask_rows.append(jnp.broadcast_to(row, (g, nodes)))
    tree_mask = jnp.concatenate(mask_rows, axis=0) > 0
    order = one_hot(
        jnp.logical_and(
            lax.rem(row_a, nodes) == lax.div(col_a, g),
            lax.div(row_a, nodes) == lax.rem(col_a, g),
        )
    )

    summed = None
    for step in range(kv):
        k = turn(side, step, kv)
        lower = []
        member = jnp.logical_and(is_hub, own_k == k)
        arrive(at_heads + k, heads.at[pl.ds(0, R * per_k - 1)], member)
        arrive(at_heads + k, heads.at[pl.ds(0, R * per_k)], jnp.logical_not(member))
        for r in range(R):
            turned = heads[pl.ds(r * H + k * per_k, per_k)].reshape(hd, lanes)
            turned = contract_last(order, turned).astype(BF16)
            lower.append(
                jnp.concatenate(
                    [turned[j * nodes : (j + 1) * nodes] for j in range(g)], axis=1
                )
            )
        lower = lower[0] if R == 1 else jnp.concatenate(lower, axis=0)
        span = g * hd
        start = pl.multiple_of(k * span, span)
        if step < kv - 1:
            more = jnp.dot(lower, ow[pl.ds(start, span), :], preferred_element_type=F32)
            summed = more if summed is None else summed + more
        else:
            for p in range(pieces):
                more = jnp.dot(
                    lower,
                    ow[pl.ds(start, span), p * piece : (p + 1) * piece],
                    preferred_element_type=F32,
                )
                if summed is not None:
                    more = more + summed[:, p * piece : (p + 1) * piece]
                terms[tp, p] = more.astype(BF16)
                for d in reversed(range(1, T)):
                    done = terms.at[tp, p]
                    send_twin(done, done, at_terms + p, twins[d])
    for name in ("hidden", "gain", "query", "near"):
        ready[name].wait()
    order_of = [
        turn(side, kv - 1 - step, kv) * per_k + turn(lane_of, d, per_k)
        for step in range(kv)
        for d in reversed(range(per_k))
    ]
    squares = jnp.zeros((M, 1), F32)
    early = None
    for p in range(pieces):
        at = slice(p * piece, (p + 1) * piece)
        arrive(at_terms + p, terms.at[pl.ds(0, T - 1), p])
        summed = terms[0, p].astype(F32)
        for t in range(1, T):
            summed = summed + terms[t, p].astype(F32)
        residual = hid_ref[:, at].astype(F32) + summed
        res_ref[:, at] = residual
        squares = squares + jnp.sum(residual * residual, axis=1, keepdims=True)
        scaled = (residual * gain_ref[:, at]).astype(BF16)
        if p < pieces - 1:
            more = [
                jnp.dot(scaled, weight[c, at, :], preferred_element_type=F32) for c in order_of
            ]
            more.append(jnp.dot(scaled, near_weight[at, :], preferred_element_type=F32))
            early = more if early is None else [x + y for x, y in zip(early, more)]

    squares = jnp.broadcast_to(squares, (M, hd))
    coarse = squares.astype(BF16).astype(F32)
    lane = lax.broadcasted_iota(jnp.int32, (M, hd), 1)
    squares = jnp.where(jnp.bitwise_and(lane, 1) == 0, coarse, squares - coarse)
    upside = lax.broadcasted_iota(jnp.int32, (nodes // 2, hd), 1) < hd // 2
    for r in range(R):
        top = squares[r * nodes : r * nodes + nodes // 2]
        bottom = squares[r * nodes + nodes // 2 : (r + 1) * nodes]
        square[r] = jnp.where(upside, top, bottom).astype(BF16)
        for step in range(kv):
            for d in reversed(range(per_k)):
                c = turn(side, kv - 1 - step, kv) * per_k + turn(lane_of, d, per_k)
                target = hub(r, c)
                send(square.at[r], gsquare.at[me], 3, target, target != me)
    for i, c in enumerate(order_of):
        out = jnp.dot(scaled, weight[c, at, :], preferred_element_type=F32)
        if early is not None:
            out = out + early[i]
        out = out.astype(BF16)
        for r in range(R):
            proj[r * H + c] = out[r * nodes : (r + 1) * nodes]
            target = hub(r, c)
            send(proj.at[r * H + c], gproj.at[me], 4, target, target != me)
    out = jnp.dot(scaled, near_weight[at, :], preferred_element_type=F32)
    if early is not None:
        out = out + early[H]
    out = out.astype(BF16)
    for r in range(R):
        for c in range(H):
            near_proj[r * H + c] = out[r * nodes : (r + 1) * nodes, c * kcols : (c + 1) * kcols]
            target = hub(r, c)
            send(near_proj.at[r * H + c], near_gproj.at[me], 5, target, target != me)

    @pl.when(is_hub)
    def _():
        gsquare[me] = square[request]
        gproj[me] = proj[request * H + slot]
        arrive(3, gsquare.at[pl.ds(0, S - 1)])
        total = gsquare[0].astype(F32)
        for s in range(1, S):
            total = total + gsquare[s].astype(F32)
        total = total + pltpu.roll(total, hd - 1, 1)
        total = jnp.concatenate(
            [jnp.broadcast_to(total[:, at : at + 1], total.shape) for at in (0, hd // 2)], axis=0
        )
        inverse = lax.rsqrt(total / width + norm_epsilon)
        arrive(4, gproj.at[pl.ds(0, S - 1)])
        inverse_ref[...] = inverse
        for t in range(qcols // hd):
            at = slice(t * hd, (t + 1) * hd)
            total = gproj[0, :, at].astype(F32)
            for s in range(1, S):
                total = total + gproj[s, :, at].astype(F32)
            upper[slot, :, at] = (total * inverse).astype(BF16)

    for d in reversed(range(1, G)):
        done = upper.at[slot]
        send(done, done, at_upper + own_k, base + mates[d], is_hub)

    @pl.when(is_hub)
    def _():
        near_gproj[me] = near_proj[request * H + slot]
        arrive(5, near_gproj.at[pl.ds(0, S - 1)])
        total = near_gproj[0].astype(F32)
        for s in range(1, S):
            total = total + near_gproj[s].astype(F32)
        inverse = jnp.concatenate([inverse_ref[...]] * (kcols // hd), axis=1)
        near_upper[slot] = (total * inverse).astype(BF16)

    for d in reversed(range(1, G)):
        done = near_upper.at[slot]
        send(done, done, 6, base + mates[d], is_hub)

    spot = lax.broadcasted_iota(jnp.int32, (lanes, hd), 1)
    third = hd // 8
    low_rows = rows // 2

    def pack_stats(stats):
        packed = jnp.zeros((lanes, hd), F32)
        at = jnp.bitwise_and(spot, third - 1)
        for i, x in enumerate(stats):
            packed = jnp.where(at == i, x, packed)
        coarse = packed.astype(BF16).astype(F32)
        rest = packed - coarse
        middle = rest.astype(BF16).astype(F32)
        fine = rest - middle
        packed = jnp.where(spot < third, coarse, jnp.where(spot < 2 * third, middle, fine))
        return jnp.where(spot < 3 * third, packed, 0.0)

    def unpack_stats(block):
        packed = block.astype(F32)
        return (packed + pltpu.roll(packed, hd - third, 1)) + pltpu.roll(
            packed, hd - 2 * third, 1
        )

    pick = one_hot(
        jnp.logical_and(
            lax.div(lax.broadcasted_iota(jnp.int32, (rows, lanes), 0), g) + place * own
            == lax.rem(lax.broadcasted_iota(jnp.int32, (rows, lanes), 1), nodes),
            lax.rem(lax.broadcasted_iota(jnp.int32, (rows, lanes), 0), g)
            == lax.div(lax.broadcasted_iota(jnp.int32, (rows, lanes), 1), nodes),
        )
    )

    def upper_queries(k):
        tiles = []
        for j in range(g):
            tile = upper[k * per_k + j // hub_heads]
            tiles.append(tile[:, (j % hub_heads) * hd : (j % hub_heads + 1) * hd])
        return jnp.concatenate(tiles, axis=0)

    stats = []
    for step in range(kv):
        k = turn(side, step, kv)
        member = jnp.logical_and(is_hub, own_k == k)
        arrive(at_upper + k, upper.at[pl.ds(0, per_k - 1)], member)
        arrive(at_upper + k, upper.at[pl.ds(0, per_k)], jnp.logical_not(member))
        queries = upper_queries(k)
        cuts = [pl.ds(p * (entries // 2), entries // 2) for p in range(2)]
        scores = [
            contract_last(queries, rkeys[k, cut, :]) + bias_ref[k, 0:1, cut] for cut in cuts
        ]
        high = jnp.max(jnp.maximum(*scores), axis=1, keepdims=True)
        high = jnp.maximum(high, lowest_high)
        blend = sum(
            jnp.dot(
                jnp.exp2((x - high) * sharp).astype(BF16),
                rvals[k, cut, :],
                preferred_element_type=F32,
            )
            for x, cut in zip(scores, cuts)
        )
        stats += [high, blend[:, hd:]]
        form[step] = blend[:, :hd]
        fresh = [step]
        if step == kv - 1:
            form[kv] = pack_stats(stats)
            fresh.append(kv)
        for a in range(G):
            for i in fresh:
                tile = [form[i, pl.ds(a * own + b, g, stride=nodes), :] for b in range(own)]
                tile = jnp.concatenate(tile, axis=0)
                if i == kv:
                    tile = jnp.where(
                        spot[:low_rows] < hd // 2,
                        tile[:low_rows],
                        pltpu.roll(tile[low_rows:], hd // 2, 1),
                    )
                upart[a, i * rows : i * rows + tile.shape[0], :] = tile.astype(BF16)
        block = pl.ds(step * rows, rows if step < kv - 1 else rows + low_rows)
        for d in reversed(range(1, G)):
            target = mates[d]
            send(upart.at[target, block], ugpart.at[place, block], 7, base + target)
    ugpart[place] = upart[place]

    arrive(6, near_upper.at[pl.ds(0, H)], jnp.logical_not(is_hub))
    arrive(6, near_upper.at[pl.ds(0, H - 1)], is_hub)
    trees = []
    for k in range(kv):
        queries = jnp.dot(pick, upper_queries(k), preferred_element_type=F32).astype(BF16)
        at = k * hd % kcols
        keys = near_upper[k * hd // kcols, :, at : at + hd]
        values = near_upper[H // 2 + k * hd // kcols, :, at : at + hd]
        scores = jnp.where(tree_mask, contract_last(queries, keys), masked_score)
        high = jnp.max(scores, axis=1, keepdims=True)
        mass = jnp.exp2((scores - high) * sharp)
        total = jnp.sum(mass, axis=1, keepdims=True)
        trees.append((jnp.dot(mass.astype(BF16), values, preferred_element_type=F32), high, total))
    arrive(7, ugpart.at[pl.ds(0, G - 1)])
    packs = []
    for s in range(G):
        pack = unpack_stats(ugpart[s, kv * rows :])
        packs.append(jnp.concatenate([pack, pltpu.roll(pack, hd // 2, 1)], axis=0))
    for k in range(kv):
        blend, high, total = trees[k]
        steps = [(k - s // (G // 2)) % kv for s in range(G)]
        stats = [
            x if step == 0 else pltpu.roll(x, hd - 2 * step, 1) for x, step in zip(packs, steps)
        ]
        top = jnp.maximum(functools.reduce(jnp.maximum, stats)[:, 0:1], high)
        late = jnp.exp2((high - top) * sharp)
        acc = blend * late
        whole = total * late
        mass = jnp.zeros((rows, hd), F32)
        for s, step in enumerate(steps):
            factor = jnp.exp2((stats[s] - top) * sharp)
            acc = acc + ugpart[s, step * rows : (step + 1) * rows].astype(F32) * factor[:, 0:1]
            mass = mass + pltpu.roll(stats[s], hd - 1, 1) * factor
        form[k, :rows, :] = acc / (whole + mass[:, 0:1])
        for j in range(g):
            h = k * g + j
            up_ref[:, h * hd : (h + 1) * hd] = form[k, pl.ds(j, own, stride=g), :]
    unit = 2 * hd
    query_bytes = 2 * kv * rows * hd
    fixed = (S - 1) * query_bytes + 2 * (T - 1) * M * features
    fixed = fixed + 2 * (G - 1) * (kv * rows + low_rows) * hd
    out_bytes = 2 * (slab + 8) * lanes + nodes * hd + 2 * nodes * (qcols + kcols)
    hub_bytes = 2 * (S - 1) * slab * lanes + 2 * (G - 1) * nodes * (qcols + kcols)
    tree_bytes = 2 * rows * hd
    plain = fixed + R * H * out_bytes + H * tree_bytes
    busy = fixed + (R * H - 1) * out_bytes + (H - 1) * tree_bytes + hub_bytes

    def gone(count):
        block = cache.at[pl.ds(0, count // unit)]
        remote(block, block, 0, peers[1]).wait_send()

    pl.when(is_hub)(lambda: gone(busy))
    pl.when(jnp.logical_not(is_hub))(lambda: gone(plain))


def shards(
    tree_hidden,
    query_low,
    key_tree_low,
    value_tree_low,
    cache_keys,
    cache_values,
    cache_lengths,
    ancestors,
    out_weight,
    norm_gain,
    w_query_up,
    w_key_up,
    w_value_up,
    retained_keys,
    retained_values,
    retained_index,
):
    S = lax.axis_size("seq")
    T = lax.axis_size("tp")
    R, part, kv, hd = cache_keys.shape
    own, row_width = query_low.shape
    g = row_width // (kv * hd)
    G = S // R
    M = S * own
    rows = own * g
    features = tree_hidden.shape[1]
    entries = retained_keys.shape[1] * kv
    ck = cache_keys.reshape(R * part * kv, hd)
    cv = cache_values.reshape(R * part * kv, hd)
    rk = retained_keys.reshape(entries, hd)
    rv = retained_values.reshape(entries, hd)
    ridx = retained_index[0].T
    gain = norm_gain.reshape(1, features)
    vmem = pl.BlockSpec(memory_space=pltpu.VMEM)
    hbm = pl.BlockSpec(memory_space=pl.ANY)
    H = G // 2
    columns = part
    pieces = 2
    big = (
        query_low,
        key_tree_low,
        value_tree_low,
        ck,
        cv,
        ancestors,
        out_weight,
        tree_hidden,
        gain,
        ridx,
        rk,
        rv,
    )
    qcols = kv * g * hd // H
    kcols = 2 * kv * hd // H
    nodes = G * own
    lanes = nodes * g
    slab = hd * kv // H
    outs = pl.pallas_call(
        functools.partial(kernel, (S, T, R, own, kv, g, hd)),
        out_shape=(
            pltpu.VMEM((M, features), F32),
            pltpu.VMEM((own, row_width), F32),
        ),
        in_specs=[hbm] * (4 + len(big)),
        out_specs=(vmem, vmem),
        scratch_shapes=[pltpu.SMEM((R,), jnp.int32)]
        + [pltpu.VMEM(x.shape, x.dtype) for x in (ancestors, out_weight, tree_hidden, gain, ridx)]
        + [
            pltpu.VMEM((own, row_width + 2 * kv * hd), BF16),
            pltpu.VMEM((2 * ck.shape[0], hd), BF16),
            pltpu.VMEM((2,) + rk.shape, BF16),
            pltpu.VMEM((H, features, qcols), BF16),
            pltpu.VMEM((features, 2 * kv * hd), BF16),
            pltpu.VMEM((kv + 1, lanes, hd), F32),
            pltpu.VMEM((max(columns * kv, entries), hd), F32),
            pltpu.VMEM((R * kv * columns, 2 * hd), BF16),
            pltpu.VMEM((R, kv, hd + 16, columns), BF16),
            pltpu.VMEM((kv, entries // kv, hd), BF16),
            pltpu.VMEM((kv, entries // kv, 2 * hd), BF16),
            pltpu.VMEM((kv, 8, entries // kv), F32),
            pltpu.VMEM((S, kv + 1, rows, hd), BF16),
            pltpu.VMEM((R * H, slab + 8, lanes), BF16),
            pltpu.VMEM((S, slab + 8, lanes), BF16),
            pltpu.VMEM((S * 8, lanes), F32),
            pltpu.VMEM((S, slab, lanes), BF16),
            pltpu.VMEM((T, pieces, M, features // pieces), BF16),
            pltpu.VMEM((R * H, nodes, qcols), BF16),
            pltpu.VMEM((S, nodes, qcols), BF16),
            pltpu.VMEM((R * H, nodes, kcols), BF16),
            pltpu.VMEM((S, nodes, kcols), BF16),
            pltpu.VMEM((R, nodes // 2, hd), BF16),
            pltpu.VMEM((S, nodes // 2, hd), BF16),
            pltpu.VMEM((H, nodes, qcols), BF16),
            pltpu.VMEM((H, nodes, kcols), BF16),
            pltpu.VMEM((nodes, hd), F32),
            pltpu.VMEM((G, kv * rows + rows // 2, hd), BF16),
            pltpu.VMEM((G, kv * rows + rows // 2, hd), BF16),
            pltpu.SemaphoreType.DMA((11,)),
            pltpu.SemaphoreType.DMA,
            pltpu.SemaphoreType.DMA((8 + 2 * kv + pieces,)),
        ],
        compiler_params=pltpu.CompilerParams(
            collective_id=0, has_side_effects=True, vmem_limit_bytes=56 * 1024 * 1024,
        ),
        name="two_layers",
    )(
        cache_lengths,
        *big,
        w_key_up,
        w_value_up,
        w_query_up,
    )

    def settle(a_ref, b_ref, c_ref, d_ref, sem):
        copies = [
            pltpu.make_async_copy(b_ref, d_ref, sem.at[1]),
            pltpu.make_async_copy(a_ref, c_ref, sem.at[0]),
        ]
        for copy in copies:
            copy.start()
        for copy in copies:
            copy.wait()

    return pl.pallas_call(
        settle,
        out_shape=tuple(jax.ShapeDtypeStruct(x.shape, x.dtype) for x in outs),
        in_specs=[vmem] * 2,
        out_specs=(hbm, hbm),
        scratch_shapes=[pltpu.SemaphoreType.DMA((2,))],
        name="settle",
    )(*[pltpu.with_memory_space_constraint(x, pltpu.VMEM) for x in outs])


def solution(mesh):
    return jax.shard_map(
        shards,
        mesh=mesh,
        in_specs=(
            P(None, "seq"),
            P("seq", "tp"),
            P("seq", "tp"),
            P("seq", "tp"),
            P(None, "seq", "tp", None),
            P(None, "seq", "tp", None),
            P(),
            P(),
            P("tp", "seq"),
            P("seq"),
            P("seq", "tp"),
            P("seq", "tp"),
            P("seq", "tp"),
            P("seq", None, "tp", None),
            P("seq", None, "tp", None),
            P("seq", None, "tp"),
        ),
        out_specs=(P(None, "seq"), P("seq", "tp")),
        check_vma=False,
    )
```
